16 devices in a mesh: dp: 4 (over y, z, core), tp: 4 (over x).
Axes of the slice: x: 4, y: 2, z: 1, core: 2. Of those that a mesh axis runs over, the one named last changes fastest.
The devices are a block of a 4x4x8 slice.
Arguments:
- x: bfloat16 [512, 7168], P('dp'), parts along dimension 0
- w_gate: bfloat16 [7168, 20480], P(None, 'tp')
- w_up: bfloat16 [7168, 20480], P(None, 'tp')
- w_down: bfloat16 [20480, 7168], P('tp')
Outputs:
- output: bfloat16 [512, 7168], P('dp'), parts along dimension 0
There are 4 independent parts. The reference program is written for one: setup_inputs(seed, part) draws one part's arguments, and reference() takes and returns one part's arrays. A program takes and returns all parts, laid end to end along the dimension named above; an argument that names none is the same for every part.
All inputs are finite; a program needn't handle non-finite values.
Results may differ from the reference program's by a relative error of at most 0.016.
Values are sent between devices in bfloat16 or wider.
A program may use at most 768 MiB of HBM per device.

```python
import jax
import jax.numpy as jnp

ROWS = 128
D = 7168
FF = 20480


def setup_inputs(seed: int = 0, part: int = 0) -> dict:
    kx, kg, ku, kd = jax.random.split(jax.random.key(seed), 4)
    drawn = {
        "x": jax.random.normal(jax.random.fold_in(kx, part), (ROWS, D), jnp.float32),
        "w_gate": jax.random.normal(kg, (D, FF), jnp.float32) * D**-0.5,
        "w_up": jax.random.normal(ku, (D, FF), jnp.float32) * D**-0.5,
        "w_down": jax.random.normal(kd, (FF, D), jnp.float32) * FF**-0.5,
    }
    return {k: v.astype(jnp.bfloat16) for k, v in drawn.items()}


def reference(x, w_gate, w_up, w_down):
    gate = jnp.dot(x, w_gate, preferred_element_type=jnp.float32)
    up = jnp.dot(x, w_up, preferred_element_type=jnp.float32)
    hidden = (jax.nn.silu(gate) * up).astype(jnp.bfloat16)
    return jnp.dot(hidden, w_down, preferred_element_type=jnp.float32).astype(jnp.bfloat16)
```

```python
import functools

import jax
import jax.numpy as jnp
from jax import lax
from jax.experimental import pallas as pl
from jax.experimental.pallas import tpu as pltpu
from jax.sharding import PartitionSpec as P

MESH = pl.DeviceIdType.MESH
HB = 256
NS = 4
CB = 512
ND = 6
LAG_A = 5
LAG_F = 14
LAG_G = 20


def kernel(
    x_ref, wg_ref, wu_ref, wd_ref, y_ref,
    xbuf, wg, wu, wd, hid, acc, d2d_out, d2d_in, s1_out, s1_in, s2_out, s2_in,
    x_sem, xs_sem, xr_sem, g_sem, u_sem, d_sem, c_send, c_recv,
    s1_send, s1_recv, s2b_send, s2b_recv, s2a_send, s2a_recv, s3_send, s3_recv, s4_send, s4_recv,
):
    rows, d = x_ref.shape
    ff = wg_ref.shape[1] // 2
    n = 4
    nb = ff // HB
    np_ = d // CB
    q = rows // n
    h = q // 2
    dp, tp = lax.axis_index("dp"), lax.axis_index("tp")
    core = lax.rem(dp, 2)
    peer = {"dp": dp + 1 - 2 * core, "tp": tp}
    right = {"dp": dp, "tp": lax.rem(tp + 1, n)}
    left = {"dp": dp, "tp": lax.rem(tp + n - 1, n)}
    me_rows = pl.multiple_of(tp * q, q)
    right_rows = pl.multiple_of(lax.rem(tp + 1, n) * q, q)
    far_rows = pl.multiple_of(lax.rem(tp + 2, n) * q, q)
    left_rows = pl.multiple_of(lax.rem(tp + 3, n) * q, q)
    base = core * ff

    def gate_copy(j):
        cols = pl.ds(pl.multiple_of(base + j * HB, HB), HB)
        s = lax.rem(j, NS)
        return pltpu.make_async_copy(wg_ref.at[:, cols], wg.at[s], g_sem.at[s])

    def up_copy(j):
        cols = pl.ds(pl.multiple_of(base + j * HB, HB), HB)
        s = lax.rem(j, NS)
        return pltpu.make_async_copy(wu_ref.at[:, cols], wu.at[s], u_sem.at[s])

    def down_copy(p):
        s = lax.rem(p, ND)
        return pltpu.make_async_copy(
            wd_ref.at[pl.ds(pl.multiple_of(base, HB), ff), pl.ds(pl.multiple_of(p * CB, CB), CB)],
            wd.at[s], d_sem.at[s])

    own_x = pltpu.make_async_copy(x_ref, xbuf.at[pl.ds(0, rows)], x_sem)
    own_x.start()
    gate_copy(0).start()
    up_copy(0).start()

    barrier = pltpu.get_barrier_semaphore()
    for other in (peer, left, right):
        pl.semaphore_signal(barrier, inc=1, device_id=other, device_id_type=MESH)
    for j in range(1, NS):
        gate_copy(j).start()
        up_copy(j).start()
    pl.semaphore_wait(barrier, 3)

    peer_x = pltpu.make_async_remote_copy(
        src_ref=x_ref, dst_ref=xbuf.at[pl.ds(rows, rows)], send_sem=xs_sem, recv_sem=xr_sem,
        device_id=peer, device_id_type=MESH)
    peer_x.start()

    def gate_up(j, r0, nr):
        s = lax.rem(j, NS)
        xs = xbuf[pl.ds(r0, nr), :]
        g = jnp.dot(xs, wg[s], preferred_element_type=jnp.float32)
        u = jnp.dot(xs, wu[s], preferred_element_type=jnp.float32)
        hid[pl.ds(r0, nr), pl.ds(pl.multiple_of(j * HB, HB), HB)] = (jax.nn.silu(g) * u).astype(hid.dtype)

    own_x.wait()
    gate_copy(0).wait()
    up_copy(0).wait()
    gate_up(0, 0, rows)
    peer_x.wait_recv()
    gate_up(0, rows, rows)
    gate_copy(NS).start()
    up_copy(NS).start()

    for p in range(ND):
        down_copy(p).start()

    @pl.loop(1, nb)
    def _(j):
        gate_copy(j).wait()
        up_copy(j).wait()
        gate_up(j, 0, 2 * rows)

        @pl.when(j + NS < nb)
        def _():
            gate_copy(j + NS).start()
            up_copy(j + NS).start()

    def cols_of(p):
        return pl.ds(pl.multiple_of(p * CB, CB), CB)

    def rcopy(src, dst, send, recv, to):
        return pltpu.make_async_remote_copy(
            src_ref=src, dst_ref=dst, send_sem=send, recv_sem=recv, device_id=to, device_id_type=MESH)

    def pair_copy(p):
        c = cols_of(p)
        return rcopy(d2d_out.at[:, c], d2d_in.at[:, c], c_send.at[p], c_recv.at[p], peer)

    def first_hop(p):
        c = cols_of(p)
        return [rcopy(s1_out.at[i, :, c], s1_in.at[i, :, c], s1_send.at[i, p], s1_recv.at[i, p], to)
                for i, to in enumerate((right, left))]

    def second_hop(p, summed):
        c = cols_of(p)
        out = []
        for i, to in enumerate((right, left)):
            r = pl.ds(h * ((i + (0 if summed else 1)) % 2), h)
            send, recv = (s2a_send, s2a_recv) if summed else (s2b_send, s2b_recv)
            out.append(rcopy(s2_out.at[i, r, c], s2_in.at[i, r, c], send.at[i, p], recv.at[i, p], to))
        return out

    def finished(p, send_side=True):
        c = cols_of(p)
        r = pl.ds(me_rows, q)
        return [rcopy(y_ref.at[r, c], y_ref.at[r, c], s3_send.at[i, p], s3_recv.at[i, p], to)
                for i, to in enumerate((right, left))]

    def forward(p):
        c = cols_of(p)
        ra = pl.ds(pl.multiple_of(left_rows, h), h)
        rb = pl.ds(pl.multiple_of(right_rows + h, h), h)
        return [rcopy(y_ref.at[r, c], y_ref.at[r, c], s4_send.at[i, p], s4_recv.at[i, p], to)
                for i, (r, to) in enumerate(((ra, right), (rb, left)))]

    @pl.loop(0, np_ + LAG_G)
    def _(it):
        @pl.when(it < np_)
        def _():
            p = it
            c = cols_of(p)
            down_copy(p).wait()
            t = jnp.dot(hid[...], wd[lax.rem(p, ND)], preferred_element_type=jnp.float32)
            d2d_out[:, c] = t[rows:].astype(d2d_out.dtype)
            acc[:, c] = t[:rows]
            pair_copy(p).start()

            @pl.when(p + ND < np_)
            def _():
                down_copy(p + ND).start()

        @pl.when((it >= 1) & (it < np_ + 1))
        def _():
            p = it - 1
            c = cols_of(p)
            pair_copy(p).wait_recv()
            acc[:, c] += d2d_in[:, c].astype(jnp.float32)
            s1_out[0, :, c] = acc[pl.ds(far_rows, h), c].astype(s1_out.dtype)
            s1_out[1, :, c] = acc[pl.ds(pl.multiple_of(far_rows + h, h), h), c].astype(s1_out.dtype)
            s2_out[0, pl.ds(h, h), c] = acc[pl.ds(pl.multiple_of(right_rows + h, h), h), c].astype(s2_out.dtype)
            s2_out[1, pl.ds(0, h), c] = acc[pl.ds(left_rows, h), c].astype(s2_out.dtype)
            for cp in first_hop(p) + second_hop(p, False):
                cp.start()

        @pl.when((it >= LAG_A) & (it < np_ + LAG_A))
        def _():
            p = it - LAG_A
            c = cols_of(p)
            for cp in first_hop(p):
                cp.wait_recv()
            s2_out[0, pl.ds(0, h), c] = (
                acc[pl.ds(right_rows, h), c] + s1_in[0, :, c].astype(jnp.float32)).astype(s2_out.dtype)
            s2_out[1, pl.ds(h, h), c] = (
                acc[pl.ds(pl.multiple_of(left_rows + h, h), h), c] + s1_in[1, :, c].astype(jnp.float32)
            ).astype(s2_out.dtype)
            for cp in second_hop(p, True):
                cp.start()

        @pl.when((it >= LAG_F) & (it < np_ + LAG_F))
        def _():
            p = it - LAG_F
            c = cols_of(p)
            for cp in second_hop(p, False) + second_hop(p, True):
                cp.wait_recv()
            y_ref[pl.ds(me_rows, q), c] = (
                acc[pl.ds(me_rows, q), c] + s2_in[0, :, c].astype(jnp.float32)
                + s2_in[1, :, c].astype(jnp.float32)).astype(y_ref.dtype)
            for cp in finished(p):
                cp.start()

        @pl.when(it >= LAG_G)
        def _():
            p = it - LAG_G
            for cp in finished(p):
                cp.wait_recv()
            for cp in forward(p):
                cp.start()

    peer_x.wait_send()

    @pl.loop(0, np_)
    def _(p):
        pair_copy(p).wait_send()
        for cp in first_hop(p) + second_hop(p, False) + second_hop(p, True) + finished(p):
            cp.wait_send()
        for cp in forward(p):
            cp.wait()


def solution(mesh):
    def step(x, w_gate, w_up, w_down):
        rows, d = x.shape
        ff = w_gate.shape[1] // 2
        q = rows // mesh.shape["tp"]
        np_ = d // CB
        bf, f32 = jnp.bfloat16, jnp.float32
        dma = pltpu.SemaphoreType.DMA
        hbm = pl.BlockSpec(memory_space=pl.ANY)
        return pl.pallas_call(
            kernel,
            out_shape=jax.ShapeDtypeStruct((rows, d), x.dtype),
            in_specs=[hbm] * 4,
            out_specs=pl.BlockSpec(memory_space=pltpu.VMEM),
            scratch_shapes=[
                pltpu.VMEM((2 * rows, d), bf),
                pltpu.VMEM((NS, d, HB), bf),
                pltpu.VMEM((NS, d, HB), bf),
                pltpu.VMEM((ND, ff, CB), bf),
                pltpu.VMEM((2 * rows, ff), bf),
                pltpu.VMEM((rows, d), f32),
                pltpu.VMEM((rows, d), bf),
                pltpu.VMEM((rows, d), bf),
                pltpu.VMEM((2, q // 2, d), bf),
                pltpu.VMEM((2, q // 2, d), bf),
                pltpu.VMEM((2, q, d), bf),
                pltpu.VMEM((2, q, d), bf),
                dma, dma, dma, dma((NS,)), dma((NS,)), dma((ND,)), dma((np_,)), dma((np_,)),
            ] + [dma((2, np_))] * 10,
            compiler_params=pltpu.CompilerParams(
                collective_id=0, has_side_effects=True, vmem_limit_bytes=67043328),
        )(x, w_gate, w_up, w_down)

    return jax.shard_map(
        step,
        mesh=mesh,
        in_specs=(P("dp", None), P(None, "tp"), P(None, "tp"), P("tp", None)),
        out_specs=P("dp", None),
        check_vma=False,
    )
```

```python
import jax
import jax.numpy as jnp
from jax import lax
from jax.experimental import pallas as pl
from jax.experimental.pallas import tpu as pltpu
from jax.sharding import PartitionSpec as P

MESH = pl.DeviceIdType.MESH
F32 = jnp.float32
HB = 256
NS = 4
OWN = 2
CB = 512
ND = 3
LB = 2
LF = 7
LG = 11


def kernel(
    x_ref, wg_ref, wu_ref, wd_ref, y_ref,
    xbuf, wg, wu, wd, hid, k_me, k_n, a_out, a_in, b_out, b_in, f_out,
    x_sem, xs_sem, xr_sem, g_sem, u_sem, d_sem, h_send, h_recv,
    a_send, a_recv, b_send, b_recv, f_send, f_recv, l_send, l_recv, g_send, g_recv,
):
    rows, d = x_ref.shape
    ff = wg_ref.shape[1] // 2
    dh = d // 2
    n = 4
    nb = ff // HB
    nc = dh // CB
    q = rows // n
    h = q // 2
    dp, tp = lax.axis_index("dp"), lax.axis_index("tp")
    core = lax.rem(dp, 2)
    other = 1 - core
    dp_peer = dp + 1 - 2 * core
    tp_r, tp_f, tp_l = [lax.rem(tp + i, n) for i in (1, 2, 3)]
    peer = {"dp": dp_peer, "tp": tp}
    side = [{"dp": dp, "tp": tp_r}, {"dp": dp, "tp": tp_l}]
    side_peer = [{"dp": dp_peer, "tp": tp_r}, {"dp": dp_peer, "tp": tp_l}]
    base = core * ff
    cbase = core * dh
    own_r = pl.multiple_of(core * rows, rows)
    peer_r = pl.multiple_of(other * rows, rows)

    def remote(src, dst, send, recv, to):
        return pltpu.make_async_remote_copy(
            src_ref=src, dst_ref=dst, send_sem=send, recv_sem=recv, device_id=to, device_id_type=MESH)

    def hcols(j):
        return pl.ds(pl.multiple_of(base + j * HB, HB), HB)

    def gate_copy(j):
        s = lax.rem(j, NS)
        return pltpu.make_async_copy(wg_ref.at[:, hcols(j)], wg.at[s], g_sem.at[s])

    def up_copy(j):
        s = lax.rem(j, NS)
        return pltpu.make_async_copy(wu_ref.at[:, hcols(j)], wu.at[s], u_sem.at[s])

    def down_copy(m):
        s = lax.rem(m, ND)
        src = wd_ref.at[:, pl.ds(pl.multiple_of(cbase + m * CB, CB), CB)]
        return pltpu.make_async_copy(src, wd.at[s], d_sem.at[s])

    def hid_copy(j):
        return remote(hid.at[:, hcols(j)], hid.at[:, hcols(j)], h_send.at[j], h_recv.at[j], peer)

    own_x = pltpu.make_async_copy(x_ref, xbuf.at[pl.ds(own_r, rows)], x_sem)
    own_x.start()
    gate_copy(0).start()
    up_copy(0).start()
    barrier = pltpu.get_barrier_semaphore()
    for to in [peer] + side + side_peer:
        pl.semaphore_signal(barrier, inc=1, device_id=to, device_id_type=MESH)
    for j in range(1, NS):
        gate_copy(j).start()
        up_copy(j).start()
    own_x.wait()
    pl.semaphore_wait(barrier, 5)
    peer_x = remote(xbuf.at[pl.ds(own_r, rows)], xbuf.at[pl.ds(own_r, rows)], xs_sem, xr_sem, peer)
    peer_x.start()

    def gate_up(j, r0, nr):
        s = lax.rem(j, NS)
        xs = xbuf[pl.ds(r0, nr), :]
        g = jnp.dot(xs, wg[s], preferred_element_type=F32)
        u = jnp.dot(xs, wu[s], preferred_element_type=F32)
        hid[pl.ds(r0, nr), hcols(j)] = (jax.nn.silu(g) * u).astype(hid.dtype)

    def refill(j):
        @pl.when(j + NS < nb)
        def _():
            gate_copy(j + NS).start()
            up_copy(j + NS).start()

        @pl.when(j + NS == nb)
        def _():
            for m in range(ND):
                down_copy(m).start()

    @pl.loop(0, OWN)
    def _(j):
        gate_copy(j).wait()
        up_copy(j).wait()
        gate_up(j, own_r, rows)

    peer_x.wait_recv()

    @pl.loop(0, OWN)
    def _(j):
        gate_up(j, peer_r, rows)
        refill(j)

    @pl.loop(OWN, nb)
    def _(j):
        gate_copy(j).wait()
        up_copy(j).wait()

        @pl.when(j == OWN)
        def _():
            for i in range(OWN - 1):
                hid_copy(i).start()

        hid_copy(j - 1).start()
        gate_up(j, 0, 2 * rows)
        refill(j)

    hid_copy(nb - 1).start()

    def chunk(m):
        return pl.ds(pl.multiple_of(m * CB, CB), CB)

    def ycols(c, half):
        return pl.ds(pl.multiple_of(half * dh + c * CB, CB), CB)

    def a_copies(m):
        c = chunk(m)
        return [remote(a_out.at[i, :, :, :, c], a_in.at[i, :, :, :, c], a_send.at[i, m], a_recv.at[i, m], side[i])
                for i in range(2)]

    def b_copies(m):
        c = chunk(m)
        return [remote(b_out.at[i, :, :, c], b_in.at[i, :, :, c], b_send.at[i, m], b_recv.at[i, m], side[i])
                for i in range(2)]

    me_rows = pl.ds(pl.multiple_of(tp * q, q), q)

    def f_copies(m):
        c = ycols(m, core)
        out = []
        for i in range(2):
            out.append(remote(y_ref.at[me_rows, c], y_ref.at[me_rows, c], f_send.at[i, 0, m],
                              f_recv.at[i, core, m], side[i]))
            out.append(remote(f_out.at[:, chunk(m)], y_ref.at[me_rows, c], f_send.at[i, 1, m],
                              f_recv.at[i, core, m], side_peer[i]))
        return out

    def f_waits(m):
        return [remote(y_ref.at[me_rows, ycols(m, e)], y_ref.at[me_rows, ycols(m, e)], f_send.at[i, 0, m],
                       f_recv.at[i, e, m], side[i]) for i in range(2) for e in range(2)]

    def l_copy(m):
        c = ycols(m, core)
        return remote(f_out.at[:, chunk(m)], y_ref.at[me_rows, c], l_send.at[m], l_recv.at[m], peer)

    def g_copies(m):
        bands = [pl.ds(pl.multiple_of(tp_l * q, h), h), pl.ds(pl.multiple_of(tp_r * q + h, h), h)]
        return [remote(y_ref.at[bands[i], ycols(m, e)], y_ref.at[bands[i], ycols(m, e)], g_send.at[i, e, m],
                       g_recv.at[i, e, m], side[i]) for i in range(2) for e in range(2)]

    def spread(t_ref, c):
        for g in range(2):
            r = g * rows
            k_me[g, :, c] = t_ref[pl.ds(pl.multiple_of(r + tp * q, q), q), :]
            k_n[0, g, :, c] = t_ref[pl.ds(pl.multiple_of(r + tp_r * q, h), h), :]
            k_n[1, g, :, c] = t_ref[pl.ds(pl.multiple_of(r + tp_l * q + h, h), h), :]
            a_out[0, 0, g, :, c] = t_ref[pl.ds(pl.multiple_of(r + tp_f * q, h), h), :].astype(a_out.dtype)
            a_out[1, 0, g, :, c] = t_ref[pl.ds(pl.multiple_of(r + tp_f * q + h, h), h), :].astype(a_out.dtype)
            a_out[0, 1, g, :, c] = t_ref[pl.ds(pl.multiple_of(r + tp_r * q + h, h), h), :].astype(a_out.dtype)
            a_out[1, 1, g, :, c] = t_ref[pl.ds(pl.multiple_of(r + tp_l * q, h), h), :].astype(a_out.dtype)

    def down(scratch):
        for j in range(nb):
            hid_copy(j).wait_recv()

        @pl.loop(0, nc + LG)
        def _(it):
            @pl.when(it < nc)
            def _():
                m = it
                down_copy(m).wait()
                scratch[...] = jnp.dot(hid[...], wd[lax.rem(m, ND)], preferred_element_type=F32)
                spread(scratch, chunk(m))
                for cp in a_copies(m):
                    cp.start()

                @pl.when(m + ND < nc)
                def _():
                    down_copy(m + ND).start()

            @pl.when((it >= LB) & (it < nc + LB))
            def _():
                m = it - LB
                c = chunk(m)
                for cp in a_copies(m):
                    cp.wait_recv()
                for i in range(2):
                    for g in range(2):
                        b_out[i, g, :, c] = (k_n[i, g, :, c] + a_in[i, 0, g, :, c].astype(F32)).astype(b_out.dtype)
                for cp in b_copies(m):
                    cp.start()

            @pl.when((it >= LF) & (it < nc + LF))
            def _():
                m = it - LF
                c = chunk(m)
                for cp in b_copies(m):
                    cp.wait_recv()

                def total(g):
                    top = k_me[g, pl.ds(0, h), c] + b_in[0, g, :, c].astype(F32) + a_in[1, 1, g, :, c].astype(F32)
                    bot = k_me[g, pl.ds(h, h), c] + a_in[0, 1, g, :, c].astype(F32) + b_in[1, g, :, c].astype(F32)
                    return top.astype(y_ref.dtype), bot.astype(y_ref.dtype)

                top, bot = total(core)
                r = pl.multiple_of(tp * q, q)
                y_ref[pl.ds(r, h), ycols(m, core)] = top
                y_ref[pl.ds(pl.multiple_of(r + h, h), h), ycols(m, core)] = bot
                top, bot = total(other)
                f_out[pl.ds(0, h), c] = top
                f_out[pl.ds(h, h), c] = bot
                for cp in f_copies(m):
                    cp.start()
                l_copy(m).start()

            @pl.when(it >= LG)
            def _():
                m = it - LG
                for cp in f_waits(m):
                    cp.wait_recv()
                for cp in g_copies(m):
                    cp.start()

    pl.run_scoped(down, pltpu.VMEM((2 * rows, CB), F32))

    peer_x.wait_send()

    @pl.loop(0, nb)
    def _(j):
        hid_copy(j).wait_send()

    @pl.loop(0, nc)
    def _(m):
        for cp in a_copies(m) + b_copies(m) + f_copies(m):
            cp.wait_send()
        l_copy(m).wait()
        for cp in g_copies(m):
            cp.wait()


def solution(mesh):
    def step(x, w_gate, w_up, w_down):
        rows, d = x.shape
        ff = w_gate.shape[1] // 2
        dh = d // 2
        q = rows // mesh.shape["tp"]
        h = q // 2
        nb = ff // HB
        nc = dh // CB
        bf = x.dtype
        vm = pltpu.VMEM
        dma = pltpu.SemaphoreType.DMA
        hbm = pl.BlockSpec(memory_space=pl.ANY)
        return pl.pallas_call(
            kernel,
            out_shape=pltpu.VMEM((rows, d), bf),
            in_specs=[hbm] * 4,
            out_specs=pl.BlockSpec(memory_space=pltpu.VMEM),
            scratch_shapes=[
                vm((2 * rows, d), bf),
                vm((NS, d, HB), bf),
                vm((NS, d, HB), bf),
                vm((ND, 2 * ff, CB), bf),
                vm((2 * rows, 2 * ff), bf),
                vm((2, q, dh), F32),
                vm((2, 2, h, dh), F32),
                vm((2, 2, 2, h, dh), bf),
                vm((2, 2, 2, h, dh), bf),
                vm((2, 2, h, dh), bf),
                vm((2, 2, h, dh), bf),
                vm((q, dh), bf),
                dma, dma, dma, dma((NS,)), dma((NS,)), dma((ND,)), dma((nb,)), dma((nb,)),
                dma((2, nc)), dma((2, nc)), dma((2, nc)), dma((2, nc)),
                dma((2, 2, nc)), dma((2, 2, nc)), dma((nc,)), dma((nc,)), dma((2, 2, nc)), dma((2, 2, nc)),
            ],
            compiler_params=pltpu.CompilerParams(
                collective_id=0, has_side_effects=True, vmem_limit_bytes=65000000),
        )(x, w_gate, w_up, w_down)

    return jax.shard_map(
        step,
        mesh=mesh,
        in_specs=(P("dp", None), P(None, "tp"), P(None, "tp"), P("tp", None)),
        out_specs=P("dp", None),
        check_vma=False,
    )
```

```python
import jax
import jax.numpy as jnp
from jax import lax
from jax.experimental import pallas as pl
from jax.experimental.pallas import tpu as pltpu
from jax.sharding import PartitionSpec as P

MESH = pl.DeviceIdType.MESH
F32 = jnp.float32
HB = 256
KC = 2
NS = 4
CB = 512
ND = 3
LB = 3
LF = 7
LG = 11


def kernel(
    x_ref, wg_ref, wu_ref, wd_ref, y_ref,
    xbuf, wg, wu, wd, hid, k_me, k_n, a_out, a_in, b_out, b_in, f_out, part,
    x_sem, xs_sem, xr_sem, g_sem, u_sem, d_sem, h_send, h_recv,
    a_send, a_recv, b_send, b_recv, f_send, f_recv, l_send, l_recv, g_send, g_recv,
):
    rows, d = x_ref.shape
    ff = wg_ref.shape[1] // 2
    dh = d // 2
    n = 4
    nb = ff // HB
    nc = dh // CB
    q = rows // n
    h = q // 2
    kd = d // KC
    dp, tp = lax.axis_index("dp"), lax.axis_index("tp")
    core = lax.rem(dp, 2)
    other = 1 - core
    dp_peer = dp + 1 - 2 * core
    tp_r, tp_l = lax.rem(tp + 1, n), lax.rem(tp + n - 1, n)
    peer = {"dp": dp_peer, "tp": tp}
    side = [{"dp": dp, "tp": tp_r}, {"dp": dp, "tp": tp_l}]
    side_peer = [{"dp": dp_peer, "tp": tp_r}, {"dp": dp_peer, "tp": tp_l}]
    base = core * ff
    cbase = core * dh
    own_r = pl.multiple_of(core * rows, rows)
    peer_r = pl.multiple_of(other * rows, rows)

    def remote(src, dst, send, recv, to):
        return pltpu.make_async_remote_copy(
            src_ref=src, dst_ref=dst, send_sem=send, recv_sem=recv, device_id=to, device_id_type=MESH)

    def hcols(j):
        return pl.ds(pl.multiple_of(base + j * HB, HB), HB)

    def gate_up_copies(j, kc):
        s = lax.rem(j, NS)
        k = pl.ds(kc * kd, kd)
        return [pltpu.make_async_copy(wg_ref.at[k, hcols(j)], wg.at[s, k], g_sem.at[s, kc]),
                pltpu.make_async_copy(wu_ref.at[k, hcols(j)], wu.at[s, k], u_sem.at[s, kc])]

    def start_block(j):
        for kc in range(KC):
            for cp in gate_up_copies(j, kc):
                cp.start()

    def k_half(e):
        return pl.ds(pl.multiple_of((core if e == 0 else other) * ff, HB), ff)

    def down_copies(m):
        s = lax.rem(m, ND)
        c = pl.ds(pl.multiple_of(cbase + m * CB, CB), CB)
        return [pltpu.make_async_copy(wd_ref.at[k_half(e), c], wd.at[s, k_half(e)], d_sem.at[s, e])
                for e in range(2)]

    def hid_copy(j):
        b = core * nb + j
        return remote(hid.at[b], hid.at[b], h_send.at[j], h_recv.at[j], peer)

    own_x = [pltpu.make_async_copy(
        x_ref.at[pl.ds(pl.multiple_of(lax.rem(tp + i, n) * q, q), q)],
        xbuf.at[pl.ds(pl.multiple_of(own_r + i * q, q), q)], x_sem.at[i]) for i in range(n)]
    for cp in own_x:
        cp.start()
    start_block(0)
    barrier = pltpu.get_barrier_semaphore()
    for to in [peer] + side + side_peer:
        pl.semaphore_signal(barrier, inc=1, device_id=to, device_id_type=MESH)
    for j in range(1, NS):
        start_block(j)
    for cp in own_x:
        cp.wait()
    pl.semaphore_wait(barrier, 5)
    peer_x = remote(xbuf.at[pl.ds(own_r, rows)], xbuf.at[pl.ds(own_r, rows)], xs_sem, xr_sem, peer)
    peer_x.start()

    def chunk(m):
        return pl.ds(pl.multiple_of(m * CB, CB), CB)

    def ycols(c, half):
        return pl.ds(pl.multiple_of(half * dh + c * CB, CB), CB)

    def a_copies(m):
        return [remote(a_out.at[i, m], a_in.at[i, m], a_send.at[i, m], a_recv.at[i, m], side[i]) for i in range(2)]

    def b_copies(m):
        return [remote(b_out.at[i, m], b_in.at[i, m], b_send.at[i, m], b_recv.at[i, m], side[i]) for i in range(2)]

    me_rows = pl.ds(pl.multiple_of(tp * q, q), q)

    def f_copies(m):
        c = ycols(m, core)
        out = []
        for i in range(2):
            out.append(remote(y_ref.at[me_rows, c], y_ref.at[me_rows, c], f_send.at[i, 0, m],
                              f_recv.at[i, core, m], side[i]))
            out.append(remote(f_out.at[m], y_ref.at[me_rows, c], f_send.at[i, 1, m],
                              f_recv.at[i, core, m], side_peer[i]))
        return out

    def f_waits(m):
        return [remote(y_ref.at[me_rows, ycols(m, e)], y_ref.at[me_rows, ycols(m, e)], f_send.at[i, 0, m],
                       f_recv.at[i, e, m], side[i]) for i in range(2) for e in range(2)]

    def l_copy(m):
        return remote(f_out.at[m], y_ref.at[me_rows, ycols(m, core)], l_send.at[m], l_recv.at[m], peer)

    def g_copies(m):
        bands = [pl.ds(pl.multiple_of(tp_l * q, h), h), pl.ds(pl.multiple_of(tp_r * q + h, h), h)]
        return [remote(y_ref.at[bands[i], ycols(m, e)], y_ref.at[bands[i], ycols(m, e)], g_send.at[i, e, m],
                       g_recv.at[i, e, m], side[i]) for i in range(2) for e in range(2)]

    def gate_up(j, r0, nr):
        s = lax.rem(j, NS)
        xs = xbuf[pl.ds(r0, nr), :]
        g = jnp.dot(xs, wg[s], preferred_element_type=F32)
        u = jnp.dot(xs, wu[s], preferred_element_type=F32)
        hid[core * nb + j, pl.ds(r0, nr)] = (jax.nn.silu(g) * u).astype(hid.dtype)

    def wait_block(j, kc):
        for cp in gate_up_copies(j, kc):
            cp.wait()

    def refill(j):
        @pl.when(j + NS < nb)
        def _():
            start_block(j + NS)

        @pl.when(j + NS == nb)
        def _():
            for m in range(ND):
                for cp in down_copies(m):
                    cp.start()

    for kc in range(KC):
        wait_block(0, kc)
    gate_up(0, own_r, rows)
    peer_x.wait_recv()
    gate_up(0, peer_r, rows)
    refill(0)

    @pl.loop(1, nb - 1)
    def _(j):
        for kc in range(KC):
            wait_block(j, kc)
        hid_copy(j - 1).start()
        gate_up(j, 0, 2 * rows)
        refill(j)

    last = nb - 1
    sl = last % NS
    for kc in range(KC):
        wait_block(last, kc)
        if kc == 0:
            hid_copy(last - 1).start()
        k = pl.ds(kc * kd, kd)
        g = jnp.dot(xbuf[:, k], wg[sl, k, :], preferred_element_type=F32)
        u = jnp.dot(xbuf[:, k], wu[sl, k, :], preferred_element_type=F32)
        if kc > 0:
            g += part[:, pl.ds(0, HB)]
            u += part[:, pl.ds(HB, HB)]
        if kc < KC - 1:
            part[:, pl.ds(0, HB)] = g
            part[:, pl.ds(HB, HB)] = u
    hid[core * nb + last] = (jax.nn.silu(g) * u).astype(hid.dtype)
    hid_copy(last).start()

    def spread(m, t):
        tb = t.astype(a_out.dtype)
        for g in range(2):
            r = g * rows
            k_me[m, g] = t[r:r + q]
            k_n[m, 0, g] = t[r + q:r + q + h]
            k_n[m, 1, g] = t[r + 3 * q + h:r + 4 * q]
            a_out[0, m, pl.ds(g * h, h)] = tb[r + 2 * q:r + 2 * q + h]
            a_out[1, m, pl.ds(g * h, h)] = tb[r + 2 * q + h:r + 3 * q]
            a_out[0, m, pl.ds((2 + g) * h, h)] = tb[r + q + h:r + 2 * q]
            a_out[1, m, pl.ds((2 + g) * h, h)] = tb[r + 3 * q:r + 3 * q + h]

    def first_hop(m):
        for cp in a_copies(m):
            cp.start()

    def second_hop(m):
        for cp in a_copies(m):
            cp.wait_recv()
        for i in range(2):
            for g in range(2):
                r = pl.ds(g * h, h)
                b_out[i, m, r] = (k_n[m, i, g] + a_in[i, m, r].astype(F32)).astype(b_out.dtype)
        for cp in b_copies(m):
            cp.start()

    def finish(m):
        for cp in b_copies(m):
            cp.wait_recv()

        def total(g):
            g0 = pl.ds(pl.multiple_of(g * h, h), h)
            g1 = pl.ds(pl.multiple_of((2 + g) * h, h), h)
            top = k_me[m, g, pl.ds(0, h)] + b_in[0, m, g0].astype(F32) + a_in[1, m, g1].astype(F32)
            bot = k_me[m, g, pl.ds(h, h)] + a_in[0, m, g1].astype(F32) + b_in[1, m, g0].astype(F32)
            return top.astype(y_ref.dtype), bot.astype(y_ref.dtype)

        top, bot = total(core)
        r = pl.multiple_of(tp * q, q)
        y_ref[pl.ds(r, h), ycols(m, core)] = top
        y_ref[pl.ds(pl.multiple_of(r + h, h), h), ycols(m, core)] = bot
        top, bot = total(other)
        f_out[m, pl.ds(0, h)] = top
        f_out[m, pl.ds(h, h)] = bot
        for cp in f_copies(m):
            cp.start()
        l_copy(m).start()

    def forward(m):
        for cp in f_waits(m):
            cp.wait_recv()
        for cp in g_copies(m):
            cp.start()

    def refill_down(m):
        @pl.when(m + ND < nc)
        def _():
            for cp in down_copies(m + ND):
                cp.start()

    def hidden(first, count):
        return jnp.concatenate([hid[first + b] for b in range(count)], axis=1)

    def down_part(e, b0, count):
        who = core if e == 0 else other
        k = pl.ds(pl.multiple_of(who * ff + b0 * HB, HB), count * HB)
        return jnp.dot(hidden(who * nb + b0, count), wd[0, k], preferred_element_type=F32)

    down_copies(0)[0].wait()
    part[...] = down_part(0, 0, nb)
    for j in range(nb - 1):
        hid_copy(j).wait_recv()
    down_copies(0)[1].wait()
    part[...] += down_part(1, 0, nb - 1)
    hid_copy(nb - 1).wait_recv()
    spread(0, part[...] + down_part(1, nb - 1, 1))
    first_hop(0)
    refill_down(0)

    @pl.loop(1, nc + LG)
    def _(it):
        @pl.when(it < nc)
        def _():
            for cp in down_copies(it):
                cp.wait()
            spread(it, jnp.dot(hidden(0, 2 * nb), wd[lax.rem(it, ND)], preferred_element_type=F32))
            first_hop(it)
            refill_down(it)

        @pl.when((it >= LB) & (it < nc + LB))
        def _():
            second_hop(it - LB)

        @pl.when((it >= LF) & (it < nc + LF))
        def _():
            finish(it - LF)

        @pl.when(it >= LG)
        def _():
            forward(it - LG)

    peer_x.wait_send()

    @pl.loop(0, nb)
    def _(j):
        hid_copy(j).wait_send()

    @pl.loop(0, nc)
    def _(m):
        for cp in a_copies(m) + b_copies(m) + f_copies(m):
            cp.wait_send()
        l_copy(m).wait()
        for cp in g_copies(m):
            cp.wait()


def solution(mesh):
    def step(x, w_gate, w_up, w_down):
        rows, d = x.shape
        ff = w_gate.shape[1] // 2
        n = mesh.shape["tp"]
        q = rows // n
        h = q // 2
        nb = ff // HB
        nc = d // 2 // CB
        bf = x.dtype
        vm = pltpu.VMEM
        dma = pltpu.SemaphoreType.DMA
        hbm = pl.BlockSpec(memory_space=pl.ANY)
        return pl.pallas_call(
            kernel,
            out_shape=pltpu.VMEM((rows, d), bf),
            in_specs=[hbm] * 4,
            out_specs=pl.BlockSpec(memory_space=pltpu.VMEM),
            scratch_shapes=[
                vm((2 * rows, d), bf),
                vm((NS, d, HB), bf),
                vm((NS, d, HB), bf),
                vm((ND, 2 * ff, CB), bf),
                vm((2 * nb, 2 * rows, HB), bf),
                vm((nc, 2, q, CB), F32),
                vm((nc, 2, 2, h, CB), F32),
                vm((2, nc, 2 * q, CB), bf),
                vm((2, nc, 2 * q, CB), bf),
                vm((2, nc, q, CB), bf),
                vm((2, nc, q, CB), bf),
                vm((nc, q, CB), bf),
                vm((2 * rows, 2 * HB), F32),
                dma((n,)), dma, dma, dma((NS, KC)), dma((NS, KC)), dma((ND, 2)), dma((nb,)), dma((nb,)),
                dma((2, nc)), dma((2, nc)), dma((2, nc)), dma((2, nc)),
                dma((2, 2, nc)), dma((2, 2, nc)), dma((nc,)), dma((nc,)), dma((2, 2, nc)), dma((2, 2, nc)),
            ],
            compiler_params=pltpu.CompilerParams(
                collective_id=0, has_side_effects=True, vmem_limit_bytes=65000000),
        )(x, w_gate, w_up, w_down)

    return jax.shard_map(
        step,
        mesh=mesh,
        in_specs=(P("dp", None), P(None, "tp"), P(None, "tp"), P("tp", None)),
        out_specs=P("dp", None),
        check_vma=False,
    )
```

```python
import functools

import jax
import jax.numpy as jnp
from jax import lax
from jax.experimental import pallas as pl
from jax.experimental.pallas import tpu as pltpu
from jax.sharding import PartitionSpec as P

MESH = pl.DeviceIdType.MESH
F32 = jnp.float32
HB = 256
KC = 2
OWN = 2
NS = 4
CB = 512
ND = 3
LB = 3
LF = 7
LG = 11


def kernel(
    n, x_ref, wg_ref, wu_ref, wd_ref, y_ref,
    xbuf, wg, wu, wd, hid, k_me, k_n, a_out, a_in, b_out, b_in, f_out, part,
    x_sem, xs_sem, xr_sem, g_sem, u_sem, d_sem, h_send, h_recv,
    a_send, a_recv, b_send, b_recv, f_send, f_recv, l_send, l_recv, g_send, g_recv,
):
    rows, d = x_ref.shape
    ff = wg_ref.shape[1] // 2
    dh = d // 2
    nb = ff // HB
    nc = dh // CB
    q = rows // n
    h = q // 2
    kd = d // KC
    dp, tp = lax.axis_index("dp"), lax.axis_index("tp")
    core = lax.rem(dp, 2)
    other = 1 - core
    dp_peer = dp + 1 - 2 * core
    tp_r, tp_l = lax.rem(tp + 1, n), lax.rem(tp + n - 1, n)
    peer = {"dp": dp_peer, "tp": tp}
    side = [{"dp": dp, "tp": tp_r}, {"dp": dp, "tp": tp_l}]
    side_peer = [{"dp": dp_peer, "tp": tp_r}, {"dp": dp_peer, "tp": tp_l}]
    base = core * ff
    cbase = core * dh
    own_r = pl.multiple_of(core * rows, rows)
    peer_r = pl.multiple_of(other * rows, rows)

    def remote(src, dst, send, recv, to):
        return pltpu.make_async_remote_copy(
            src_ref=src, dst_ref=dst, send_sem=send, recv_sem=recv, device_id=to, device_id_type=MESH)

    def hcols(j):
        return pl.ds(pl.multiple_of(base + j * HB, HB), HB)

    def gate_up_copies(j, kc):
        s = lax.rem(j, NS)
        k = pl.ds(kc * kd, kd)
        return [pltpu.make_async_copy(wg_ref.at[k, hcols(j)], wg.at[s, k], g_sem.at[s, kc]),
                pltpu.make_async_copy(wu_ref.at[k, hcols(j)], wu.at[s, k], u_sem.at[s, kc])]

    def start_block(j):
        for kc in range(KC):
            for cp in gate_up_copies(j, kc):
                cp.start()

    def k_half(e):
        return pl.ds(pl.multiple_of((core if e == 0 else other) * ff, HB), ff)

    def down_copies(m):
        s = lax.rem(m, ND)
        c = pl.ds(pl.multiple_of(cbase + m * CB, CB), CB)
        return [pltpu.make_async_copy(wd_ref.at[k_half(e), c], wd.at[s, k_half(e)], d_sem.at[s, e])
                for e in range(2)]

    def hid_copy(j):
        b = core * nb + j
        return remote(hid.at[b], hid.at[b], h_send.at[j], h_recv.at[j], peer)

    own_x = [pltpu.make_async_copy(
        x_ref.at[pl.ds(pl.multiple_of(lax.rem(tp + i, n) * q, q), q)],
        xbuf.at[pl.ds(pl.multiple_of(own_r + i * q, q), q)], x_sem.at[i]) for i in range(n)]
    for cp in own_x:
        cp.start()
    start_block(0)
    barrier = pltpu.get_barrier_semaphore()
    for to in [peer] + side + side_peer:
        pl.semaphore_signal(barrier, inc=1, device_id=to, device_id_type=MESH)
    for j in range(1, NS):
        start_block(j)
    for cp in own_x:
        cp.wait()
    pl.semaphore_wait(barrier, 5)
    peer_x = remote(xbuf.at[pl.ds(own_r, rows)], xbuf.at[pl.ds(own_r, rows)], xs_sem, xr_sem, peer)
    peer_x.start()

    def chunk(m):
        return pl.ds(pl.multiple_of(m * CB, CB), CB)

    def ycols(c, half):
        return pl.ds(pl.multiple_of(half * dh + c * CB, CB), CB)

    def a_copies(m):
        return [remote(a_out.at[i, m], a_in.at[i, m], a_send.at[i, m], a_recv.at[i, m], side[i]) for i in range(2)]

    def b_copies(m):
        return [remote(b_out.at[i, m], b_in.at[i, m], b_send.at[i, m], b_recv.at[i, m], side[i]) for i in range(2)]

    me_rows = pl.ds(pl.multiple_of(tp * q, q), q)

    def f_copies(m):
        c = ycols(m, core)
        out = []
        for i in range(2):
            out.append(remote(y_ref.at[me_rows, c], y_ref.at[me_rows, c], f_send.at[i, 0, m],
                              f_recv.at[i, core, m], side[i]))
            out.append(remote(f_out.at[m], y_ref.at[me_rows, c], f_send.at[i, 1, m],
                              f_recv.at[i, core, m], side_peer[i]))
        return out

    def f_waits(m):
        return [remote(y_ref.at[me_rows, ycols(m, e)], y_ref.at[me_rows, ycols(m, e)], f_send.at[i, 0, m],
                       f_recv.at[i, e, m], side[i]) for i in range(2) for e in range(2)]

    def l_copy(m):
        return remote(f_out.at[m], y_ref.at[me_rows, ycols(m, core)], l_send.at[m], l_recv.at[m], peer)

    def g_copies(m):
        bands = [pl.ds(pl.multiple_of(tp_l * q, h), h), pl.ds(pl.multiple_of(tp_r * q + h, h), h)]
        return [remote(y_ref.at[bands[i], ycols(m, e)], y_ref.at[bands[i], ycols(m, e)], g_send.at[i, e, m],
                       g_recv.at[i, e, m], side[i]) for i in range(2) for e in range(2)]

    def gate_up(j, r0, nr):
        s = lax.rem(j, NS)
        xs = xbuf[pl.ds(r0, nr), :]
        g = jnp.dot(xs, wg[s], preferred_element_type=F32)
        u = jnp.dot(xs, wu[s], preferred_element_type=F32)
        hid[core * nb + j, pl.ds(r0, nr)] = (jax.nn.silu(g) * u).astype(hid.dtype)

    def wait_block(j, kc):
        for cp in gate_up_copies(j, kc):
            cp.wait()

    def refill(j):
        @pl.when(j + NS < nb)
        def _():
            start_block(j + NS)

        @pl.when(j + NS == nb)
        def _():
            for m in range(ND):
                for cp in down_copies(m):
                    cp.start()

    @pl.loop(0, OWN)
    def _(j):
        for kc in range(KC):
            wait_block(j, kc)
        gate_up(j, own_r, rows)

    peer_x.wait_recv()

    @pl.loop(0, OWN)
    def _(j):
        gate_up(j, peer_r, rows)
        refill(j)

    for j in range(OWN - 1):
        hid_copy(j).start()

    @pl.loop(OWN, nb - 1)
    def _(j):
        for kc in range(KC):
            wait_block(j, kc)
        hid_copy(j - 1).start()
        gate_up(j, 0, 2 * rows)
        refill(j)

    last = nb - 1
    sl = last % NS
    for kc in range(KC):
        wait_block(last, kc)
        if kc == 0:
            hid_copy(last - 1).start()
        k = pl.ds(kc * kd, kd)
        g = jnp.dot(xbuf[:, k], wg[sl, k, :], preferred_element_type=F32)
        u = jnp.dot(xbuf[:, k], wu[sl, k, :], preferred_element_type=F32)
        if kc > 0:
            g += part[:, pl.ds(0, HB)]
            u += part[:, pl.ds(HB, HB)]
        if kc < KC - 1:
            part[:, pl.ds(0, HB)] = g
            part[:, pl.ds(HB, HB)] = u
    hid[core * nb + last] = (jax.nn.silu(g) * u).astype(hid.dtype)
    hid_copy(last).start()

    def spread(m, t):
        tb = t.astype(a_out.dtype)
        for g in range(2):
            r = g * rows
            k_me[m, g] = t[r:r + q]
            k_n[m, 0, g] = t[r + q:r + q + h]
            k_n[m, 1, g] = t[r + 3 * q + h:r + 4 * q]
            a_out[0, m, pl.ds(g * h, h)] = tb[r + 2 * q:r + 2 * q + h]
            a_out[1, m, pl.ds(g * h, h)] = tb[r + 2 * q + h:r + 3 * q]
            a_out[0, m, pl.ds((2 + g) * h, h)] = tb[r + q + h:r + 2 * q]
            a_out[1, m, pl.ds((2 + g) * h, h)] = tb[r + 3 * q:r + 3 * q + h]

    def first_hop(m):
        for cp in a_copies(m):
            cp.start()

    def second_hop(m):
        for cp in a_copies(m):
            cp.wait_recv()
        for i in range(2):
            for g in range(2):
                r = pl.ds(g * h, h)
                b_out[i, m, r] = (k_n[m, i, g] + a_in[i, m, r].astype(F32)).astype(b_out.dtype)
        for cp in b_copies(m):
            cp.start()

    def finish(m):
        for cp in b_copies(m):
            cp.wait_recv()

        def total(g):
            g0 = pl.ds(pl.multiple_of(g * h, h), h)
            g1 = pl.ds(pl.multiple_of((2 + g) * h, h), h)
            top = k_me[m, g, pl.ds(0, h)] + b_in[0, m, g0].astype(F32) + a_in[1, m, g1].astype(F32)
            bot = k_me[m, g, pl.ds(h, h)] + a_in[0, m, g1].astype(F32) + b_in[1, m, g0].astype(F32)
            return top.astype(y_ref.dtype), bot.astype(y_ref.dtype)

        top, bot = total(core)
        r = pl.multiple_of(tp * q, q)
        y_ref[pl.ds(r, h), ycols(m, core)] = top
        y_ref[pl.ds(pl.multiple_of(r + h, h), h), ycols(m, core)] = bot
        top, bot = total(other)
        f_out[m, pl.ds(0, h)] = top
        f_out[m, pl.ds(h, h)] = bot
        for cp in f_copies(m):
            cp.start()
        l_copy(m).start()

    def forward(m):
        for cp in f_waits(m):
            cp.wait_recv()
        for cp in g_copies(m):
            cp.start()

    def refill_down(m):
        @pl.when(m + ND < nc)
        def _():
            for cp in down_copies(m + ND):
                cp.start()

    def hidden(first, count):
        return jnp.concatenate([hid[first + b] for b in range(count)], axis=1)

    def down_part(e, b0, count):
        who = core if e == 0 else other
        k = pl.ds(pl.multiple_of(who * ff + b0 * HB, HB), count * HB)
        return jnp.dot(hidden(who * nb + b0, count), wd[0, k], preferred_element_type=F32)

    down_copies(0)[0].wait()
    part[...] = down_part(0, 0, nb)
    for j in range(nb - 1):
        hid_copy(j).wait_recv()
    down_copies(0)[1].wait()
    part[...] += down_part(1, 0, nb - 1)
    hid_copy(nb - 1).wait_recv()
    spread(0, part[...] + down_part(1, nb - 1, 1))
    first_hop(0)
    refill_down(0)

    @pl.loop(1, nc + LG)
    def _(it):
        @pl.when(it < nc)
        def _():
            for cp in down_copies(it):
                cp.wait()
            spread(it, jnp.dot(hidden(0, 2 * nb), wd[lax.rem(it, ND)], preferred_element_type=F32))
            first_hop(it)
            refill_down(it)

        @pl.when((it >= LB) & (it < nc + LB))
        def _():
            second_hop(it - LB)

        @pl.when((it >= LF) & (it < nc + LF))
        def _():
            finish(it - LF)

        @pl.when(it >= LG)
        def _():
            forward(it - LG)

    peer_x.wait_send()

    @pl.loop(0, nb)
    def _(j):
        hid_copy(j).wait_send()

    @pl.loop(0, nc)
    def _(m):
        for cp in a_copies(m) + b_copies(m) + f_copies(m):
            cp.wait_send()
        l_copy(m).wait()
        for cp in g_copies(m):
            cp.wait()


def solution(mesh):
    def step(x, w_gate, w_up, w_down):
        rows, d = x.shape
        ff = w_gate.shape[1] // 2
        n = mesh.shape["tp"]
        q = rows // n
        h = q // 2
        nb = ff // HB
        nc = d // 2 // CB
        bf = x.dtype
        vm = pltpu.VMEM
        dma = pltpu.SemaphoreType.DMA
        hbm = pl.BlockSpec(memory_space=pl.ANY)
        return pl.pallas_call(
            functools.partial(kernel, n),
            out_shape=pltpu.VMEM((rows, d), bf),
            in_specs=[hbm] * 4,
            out_specs=pl.BlockSpec(memory_space=pltpu.VMEM),
            scratch_shapes=[
                vm((2 * rows, d), bf),
                vm((NS, d, HB), bf),
                vm((NS, d, HB), bf),
                vm((ND, 2 * ff, CB), bf),
                vm((2 * nb, 2 * rows, HB), bf),
                vm((nc, 2, q, CB), F32),
                vm((nc, 2, 2, h, CB), F32),
                vm((2, nc, 2 * q, CB), bf),
                vm((2, nc, 2 * q, CB), bf),
                vm((2, nc, q, CB), bf),
                vm((2, nc, q, CB), bf),
                vm((nc, q, CB), bf),
                vm((2 * rows, 2 * HB), F32),
                dma((n,)), dma, dma, dma((NS, KC)), dma((NS, KC)), dma((ND, 2)), dma((nb,)), dma((nb,)),
                dma((2, nc)), dma((2, nc)), dma((2, nc)), dma((2, nc)),
                dma((2, 2, nc)), dma((2, 2, nc)), dma((nc,)), dma((nc,)), dma((2, 2, nc)), dma((2, 2, nc)),
            ],
            compiler_params=pltpu.CompilerParams(
                collective_id=0, has_side_effects=True, vmem_limit_bytes=65000000),
        )(x, w_gate, w_up, w_down)

    return jax.shard_map(
        step,
        mesh=mesh,
        in_specs=(P("dp", None), P(None, "tp"), P(None, "tp"), P("tp", None)),
        out_specs=P("dp", None),
        check_vma=False,
    )
```
